32 devices in a mesh: group: 2 (over y), ha: 4 (over x, core), wa: 4 (over z).
Axes of the slice: x: 2, y: 2, z: 4, core: 2. Of those that a mesh axis runs over, the one named last changes fastest.
Arguments:
- queries: bfloat16 [4, 32, 32, 1536], P('group', 'ha', 'wa'), parts along dimension 0, may hold values from -6 to 6
- keys: bfloat16 [4, 32, 32, 1536], P('group', 'ha', 'wa'), parts along dimension 0, may hold values from -6 to 6
- values: bfloat16 [4, 32, 32, 1536], P('group', 'ha', 'wa'), parts along dimension 0, may hold values from -6 to 6
- out_grad: bfloat16 [4, 32, 32, 1536], P('group', 'ha', 'wa'), parts along dimension 0, may hold values from -96 to 96
- log_norm: float32 [12, 4, 32, 32], P(None, 'group', 'ha', 'wa'), parts along dimension 1, may hold values from 6.5 to 7.5
- delta_rows: float32 [12, 4, 32, 32], P(None, 'group', 'ha', 'wa'), parts along dimension 1, may hold values from -360 to 360
- text_keys: bfloat16 [64, 1536], P('group'), parts along dimension 0, may hold values from -6 to 6
- text_values: bfloat16 [64, 1536], P('group'), parts along dimension 0, may hold values from -6 to 6
- window_table: int32 [4, 4, 9], replicated, may hold values 0 or 1
Outputs:
- query_grad: bfloat16 [4, 32, 32, 1536], P('group', 'ha', 'wa'), parts along dimension 0
- key_grad: bfloat16 [4, 32, 32, 1536], P('group', 'ha', 'wa'), parts along dimension 0
- value_grad: bfloat16 [4, 32, 32, 1536], P('group', 'ha', 'wa'), parts along dimension 0
- text_key_grad: bfloat16 [64, 1536], P('group'), parts along dimension 0
- text_value_grad: bfloat16 [64, 1536], P('group'), parts along dimension 0
The draws below stay inside these ranges and needn't reach their ends.
There are 2 independent parts, one for each index of `group`. The reference program is written for one: setup_inputs(seed, part) draws one part's arguments, and reference() takes and returns one part's arrays. A program takes and returns all parts, laid end to end along the dimension named above; an argument that names none is the same for every part. Nothing has to cross between parts.
All inputs are finite; a program needn't handle non-finite values.
Results may differ from the reference program's by a relative error of at most 0.001.
The reference program's roundings to bfloat16 on the way (of `probs_half` and `score_grad`) count: a program that leaves them out, or rounds other values in their place, can miss the bound.
Values may be sent and summed in bfloat16 or wider, within the bound.
A program may use at most 64 MiB of HBM per device.

```python
import jax
import jax.numpy as jnp
from jax import lax

HEADS = 12
HDIM = 128
TEXT = 32
FRAMES = 2
TILE = 8
HALO = 2
HD = 1536
NH = 32
NW = 32
N_HA = 4
N_WA = 4


def place_ends(array, own_key, least, high):
    place = [jax.random.randint(jax.random.fold_in(own_key, axis), (), 0, length) for axis, length in enumerate(array.shape)]
    longest = array.shape.index(max(array.shape))
    neighbour = place[:longest] + [(place[longest] + 1) % array.shape[longest]] + place[longest + 1:]
    return array.at[tuple(place)].set(least).at[tuple(neighbour)].set(high)


def shard_levels(stream_key, dims, split, least, largest):
    gain, own = 1.0, jax.random.fold_in(stream_key, 6)
    for axis_at, shards_of in split:
        heights = jnp.exp(jax.random.uniform(jax.random.fold_in(own, axis_at), (shards_of,), jnp.float32, least / len(split), largest / len(split)))
        gain = gain * jnp.repeat(heights, dims[axis_at] // shards_of).reshape([-1 if axis == axis_at else 1 for axis in range(len(dims))])
    return gain


def gaussian(rng, dims, scale, most, shards=(), kind=jnp.bfloat16):
    drawn = jax.random.normal(rng, dims, jnp.float32) * scale
    if len(shards) > 0:
        drawn = shard_levels(rng, dims, shards, -0.22, 0.18) * drawn
    return jnp.clip(drawn, min=-most, max=most).astype(kind)


def setup_inputs(seed: int = 0, part: int = 0) -> dict:
    streams_of = jax.random.split(jax.random.key(seed), 10)
    part_keys = jax.random.split(jax.random.fold_in(streams_of[9], part), 10)
    return {
        "queries": gaussian(part_keys[0], (FRAMES, NH, NW, HD), 1.0, 6.0, ((1, 4), (2, 4))),
        "keys": gaussian(part_keys[1], (FRAMES, NH, NW, HD), 1.0, 6.0, ((1, 4), (2, 4))),
        "values": gaussian(part_keys[2], (FRAMES, NH, NW, HD), 1.0, 6.0, ((1, 4), (2, 4))),
        "out_grad": gaussian(part_keys[3], (FRAMES, NH, NW, HD), 16.0, 96.0, ((1, 4), (2, 4))),
        "log_norm": jnp.clip(6.5 + 1.0 * jax.random.uniform(part_keys[4], (HEADS, FRAMES, NH, NW), jnp.float32) ** shard_levels(part_keys[4], (HEADS, FRAMES, NH, NW), ((2, 4), (3, 4)), -0.2, 0.2), 6.5, 7.5),
        "delta_rows": gaussian(part_keys[5], (HEADS, FRAMES, NH, NW), 60.0, 360.0, ((2, 4), (3, 4)), jnp.float32),
        "text_keys": gaussian(part_keys[6], (TEXT, HD), 1.0, 6.0),
        "text_values": gaussian(part_keys[7], (TEXT, HD), 1.0, 6.0),
        "window_table": place_ends((jax.random.randint(streams_of[8], (N_HA, N_WA, 9), 0, 4) < 3).astype(jnp.int32), jax.random.fold_in(streams_of[8], 1), 0, 1),
    }


def tile_grads(query_rows, cotangent_rows, norm_rows, delta_part, key_rows, value_rows, cell_mask):
    score_scale = 1.0 / (HDIM ** 0.5)
    query_wide = query_rows.astype(jnp.float32)
    cotangent_wide = cotangent_rows.astype(jnp.float32)
    key_wide = key_rows.astype(jnp.float32)
    value_wide = value_rows.astype(jnp.float32)
    scores = jnp.einsum("qhd,khd->hqk", query_wide, key_wide) * score_scale
    probs = jnp.exp(scores - norm_rows[:, :, None])
    if cell_mask is not None:
        probs = probs * cell_mask[None, None, :]
    probs_half = probs.astype(jnp.bfloat16)
    value_part = jnp.einsum("hqk,qhd->khd", probs_half.astype(jnp.float32), cotangent_wide)
    prob_grad = jnp.einsum("qhd,khd->hqk", cotangent_wide, value_wide)
    score_grad = (probs * (prob_grad - delta_part[:, :, None])).astype(jnp.bfloat16).astype(jnp.float32)
    query_part = jnp.einsum("hqk,khd->qhd", score_grad, key_wide) * score_scale
    key_part = jnp.einsum("hqk,qhd->khd", score_grad, query_wide) * score_scale
    return query_part, key_part, value_part


def reference(queries, keys, values, out_grad, log_norm, delta_rows, text_keys, text_values, window_table):
    frames, rows_all, cols_all, width = queries.shape
    tile_side = TILE
    halo_rim = HALO
    window_side = TILE + 2 * HALO
    pad_spec = ((0, 0), (halo_rim, halo_rim), (halo_rim, halo_rim), (0, 0))
    key_pad = jnp.pad(keys, pad_spec, mode="wrap")
    value_pad = jnp.pad(values, pad_spec, mode="wrap")
    position = jnp.arange(window_side, dtype=jnp.int32)
    block_of = (position >= halo_rim).astype(jnp.int32) + (position >= halo_rim + tile_side).astype(jnp.int32)
    text_key_rows = text_keys.reshape(TEXT, HEADS, HDIM)
    text_value_rows = text_values.reshape(TEXT, HEADS, HDIM)

    def per_tile(carry, tile_index):
        grad_pad, text_total = carry
        row_tile = (tile_index // N_WA).astype(jnp.int32)
        col_tile = (tile_index % N_WA).astype(jnp.int32)
        row_start = (row_tile * tile_side).astype(jnp.int32)
        col_start = (col_tile * tile_side).astype(jnp.int32)
        anchor = jnp.zeros((), jnp.int32)
        tile_shape = (frames, tile_side, tile_side, width)
        query_rows = lax.dynamic_slice(queries, (anchor, row_start, col_start, anchor), tile_shape).reshape(-1, HEADS, HDIM)
        cotangent_rows = lax.dynamic_slice(out_grad, (anchor, row_start, col_start, anchor), tile_shape).reshape(-1, HEADS, HDIM)
        stat_shape = (HEADS, frames, tile_side, tile_side)
        norm_rows = lax.dynamic_slice(log_norm, (anchor, anchor, row_start, col_start), stat_shape).reshape(HEADS, -1)
        delta_part = lax.dynamic_slice(delta_rows, (anchor, anchor, row_start, col_start), stat_shape).reshape(HEADS, -1)
        window_shape = (frames, window_side, window_side, width)
        key_rows = lax.dynamic_slice(key_pad, (anchor, row_start, col_start, anchor), window_shape).reshape(-1, HEADS, HDIM)
        value_rows = lax.dynamic_slice(value_pad, (anchor, row_start, col_start, anchor), window_shape).reshape(-1, HEADS, HDIM)
        pattern = lax.dynamic_slice(window_table, (row_tile, col_tile, anchor), (1, 1, 9)).reshape(9).astype(jnp.float32)
        cell_grid = pattern[3 * block_of[:, None] + block_of[None, :]]
        cell_mask = jnp.broadcast_to(cell_grid[None], (frames, window_side, window_side)).reshape(-1)
        video_query, video_key, video_value = tile_grads(query_rows, cotangent_rows, norm_rows, delta_part, key_rows, value_rows, cell_mask)
        text_query, text_key, text_value = tile_grads(query_rows, cotangent_rows, norm_rows, delta_part, text_key_rows, text_value_rows, None)
        query_tile = (video_query + text_query).astype(jnp.bfloat16).reshape(tile_shape)
        window_grad = jnp.stack((video_key, video_value)).reshape((2,) + window_shape)
        start = (anchor, anchor, row_start, col_start, anchor)
        current = lax.dynamic_slice(grad_pad, start, window_grad.shape)
        grad_pad = lax.dynamic_update_slice(grad_pad, current + window_grad, start)
        text_total = text_total + jnp.stack((text_key, text_value))
        return (grad_pad, text_total), query_tile

    grad_start = jnp.zeros((2, frames, rows_all + 2 * halo_rim, cols_all + 2 * halo_rim, width), jnp.float32)
    text_start = jnp.zeros((2, TEXT, HEADS, HDIM), jnp.float32)
    (grad_pad, text_total), query_tiles = lax.scan(per_tile, (grad_start, text_start), jnp.arange(N_HA * N_WA, dtype=jnp.int32))
    folded = grad_pad[:, :, halo_rim:halo_rim + rows_all]
    folded = folded.at[:, :, :halo_rim].add(grad_pad[:, :, halo_rim + rows_all:])
    folded = folded.at[:, :, rows_all - halo_rim:].add(grad_pad[:, :, :halo_rim])
    core = folded[:, :, :, halo_rim:halo_rim + cols_all]
    core = core.at[:, :, :, :halo_rim].add(folded[:, :, :, halo_rim + cols_all:])
    core = core.at[:, :, :, cols_all - halo_rim:].add(folded[:, :, :, :halo_rim])
    query_grad = query_tiles.reshape(N_HA, N_WA, frames, tile_side, tile_side, width)
    query_grad = query_grad.transpose(2, 0, 3, 1, 4, 5).reshape(frames, rows_all, cols_all, width)
    text_key_grad = text_total[0].reshape(TEXT, HEADS * HDIM).astype(jnp.bfloat16)
    text_value_grad = text_total[1].reshape(TEXT, HEADS * HDIM).astype(jnp.bfloat16)
    return query_grad, core[0].astype(jnp.bfloat16), core[1].astype(jnp.bfloat16), text_key_grad, text_value_grad
```

```python
import functools
import math

import jax
import jax.numpy as jnp
from jax import lax
from jax.experimental import pallas as pl
from jax.experimental.pallas import tpu as pltpu
from jax.sharding import PartitionSpec as P

HDIM = 128
HALO = 2
GROUPS = 4
MESH = pl.DeviceIdType.MESH
F32 = jnp.float32
BF16 = jnp.bfloat16


def text_plan(n_ha, n_wa, blocks, width):
    plan = []
    for axis, count in (("ha", n_ha), ("wa", n_wa)):
        far = 1
        while far < count:
            if blocks > 1:
                blocks //= 2
                plan.append((axis, far, blocks, width, "rows"))
            elif width % 256 == 0:
                width //= 2
                plan.append((axis, far, blocks, width, "cols"))
            else:
                plan.append((axis, far, blocks, width, "none"))
            far *= 2
    return plan


def to_rows(block, rows):
    return block.astype(F32).reshape(rows, block.shape[-1])


def contract(a, b, dims):
    return lax.dot_general(a, b, (dims, ((), ())), preferred_element_type=F32)


def kernel(
    n_ha, n_wa, plan,
    table, q_ref, k_ref, v_ref, g_ref, norm_ref, delta_ref, tk_ref, tv_ref,
    dq_ref, dk_ref, dv_ref, dtk_ref, dtv_ref,
    stage, hcol, hrow, hcor, ret, rrow, rcol, own, dq_acc, mask, norm, delta, tx, tb, *rest,
):
    trecv = rest[: len(plan)]
    (col_s, col_r, row_s, row_r, cor_s, cor_r, rr_s, rr_r, rc_s, rc_r, t_s, t_r, u_s, u_r) = rest[len(plan):]
    frames, tile, _, width = q_ref.shape
    cells = frames * tile * tile
    text = tk_ref.shape[0]
    heads = width // HDIM
    part = width // GROUPS
    per = heads // GROUPS
    bands = tile // HALO
    scale = 1.0 / math.sqrt(HDIM)
    ha, wa = lax.axis_index("ha"), lax.axis_index("wa")
    ha_of = [{"ha": lax.rem(ha + n_ha - 1, n_ha)}, {"ha": lax.rem(ha + 1, n_ha)}]
    wa_of = [{"wa": lax.rem(wa + n_wa - 1, n_wa)}, {"wa": lax.rem(wa + 1, n_wa)}]
    partners, bits = [], []
    for axis, far, _, _, _ in plan:
        at = ha if axis == "ha" else wa
        bit = lax.rem(lax.div(at, far), 2)
        bits.append(bit)
        partners.append({axis: at + far * (1 - 2 * bit)})

    barrier = pltpu.get_barrier_semaphore()
    greeted = ha_of + wa_of + partners
    for other in greeted:
        pl.semaphore_signal(barrier, inc=1, device_id=other, device_id_type=MESH)

    def cols(g):
        return slice(g * part, (g + 1) * part)

    def remote(src, dst, s, r, device):
        return pltpu.make_async_remote_copy(
            src_ref=src, dst_ref=dst, send_sem=s, recv_sem=r, device_id=device, device_id_type=MESH
        )

    border = 2 * bands * frames * HALO * HALO

    def cell_of(j):
        side = lax.div(j, border // 2)
        band = lax.rem(lax.div(j, frames * HALO * HALO), bands)
        frame = lax.rem(lax.div(j, HALO * HALO), frames)
        row = band * HALO + lax.rem(lax.div(j, HALO), HALO)
        col = lax.rem(j, HALO) + side * (tile - HALO)
        return frame * tile * tile + row * tile + col

    lane = lax.broadcasted_iota(jnp.int32, (border, cells), 1)
    pick = (lane == cell_of(lax.broadcasted_iota(jnp.int32, (border, cells), 0))).astype(F32).astype(BF16)
    back_row = lax.broadcasted_iota(jnp.int32, (cells, 3 * border), 0)
    back_lane = lax.broadcasted_iota(jnp.int32, (cells, 3 * border), 1)
    put_back = (back_row == cell_of(lax.rem(back_lane, border))).astype(F32).astype(BF16)

    col_copy, row_copy, cor_copy, rr_copy, rc_copy = {}, {}, {}, {}, {}
    for g in range(GROUPS):
        for kv, ref in enumerate((k_ref, v_ref)):
            full = to_rows(ref[:, :, :, cols(g)], cells).astype(BF16)
            strip = contract(pick, full, ((1,), (0,)))
            stage[g, kv] = strip.reshape(2, bands, frames * HALO * HALO, part).astype(BF16)
        if g == 0:
            pl.semaphore_wait(barrier, len(greeted))
        for d in range(2):
            c = remote(stage.at[g, :, d], hcol.at[g, :, 1 - d], col_s.at[g, d], col_r.at[g, 1 - d], wa_of[d])
            c.start()
            col_copy[g, d] = c
        for v in range(2):
            for kv, ref in enumerate((k_ref, v_ref)):
                lo = v * (tile - HALO)
                c = remote(
                    ref.at[:, lo:lo + HALO, :, cols(g)], hrow.at[g, kv, 1 - v],
                    row_s.at[g, v, kv], row_r.at[g, 1 - v, kv], ha_of[v],
                )
                c.start()
                row_copy[g, v, kv] = c

    spread = (
        lax.rem(lax.broadcasted_iota(jnp.int32, (tile, cells), 1), tile)
        == lax.broadcasted_iota(jnp.int32, (tile, cells), 0)
    ).astype(F32)
    lines = frames * tile
    stat_shape = (heads * lines, cells)
    keep = lax.rem(lax.broadcasted_iota(jnp.int32, stat_shape, 0), lines) == lax.div(
        lax.broadcasted_iota(jnp.int32, stat_shape, 1), tile
    )
    for src, dst in ((norm_ref, norm), (delta_ref, delta)):
        wide = jnp.dot(src[...], spread, precision=lax.Precision.HIGHEST, preferred_element_type=F32)
        dst[...] = jnp.where(keep, wide, 0.0).reshape(heads, lines, cells).sum(axis=1)

    def live(block):
        return table[ha, wa, block].astype(F32)

    at = 0
    for block, rows in ((1, 32), (0, 8), (2, 8), (7, 32), (6, 8), (8, 8), (3, 32), (5, 32)):
        mask[at:at + rows, :] = jnp.full((rows, cells), live(block), F32)
        at += rows
    own_live = live(4)

    def attend(keys, values, h, masking):
        here = slice(h * HDIM, (h + 1) * HDIM)
        qh = to_rows(q_ref[:, :, :, here], cells).astype(BF16)
        gh = to_rows(g_ref[:, :, :, here], cells).astype(BF16)
        s = contract(keys, qh, ((1,), (1,))) * scale
        p = masking(jnp.exp(s - norm[h:h + 1, :]))
        dp = contract(values, gh, ((1,), (1,)))
        ds = (p * (dp - delta[h:h + 1, :])).astype(BF16)
        dv = contract(p.astype(BF16), gh, ((1,), (0,)))
        dk = contract(ds, qh, ((1,), (0,)))
        dq = contract(ds, keys, ((0,), (0,)))
        return dq, dk, dv

    def local(g):
        for h in range(g * per, (g + 1) * per):
            here = slice(h * HDIM, (h + 1) * HDIM)
            keys = jnp.concatenate([to_rows(k_ref[:, :, :, here], cells), tk_ref[:, here].astype(F32)], 0).astype(BF16)
            values = jnp.concatenate([to_rows(v_ref[:, :, :, here], cells), tv_ref[:, here].astype(F32)], 0).astype(BF16)
            dq, dk, dv = attend(
                keys, values, h, lambda p: jnp.concatenate([p[:cells] * own_live, p[cells:]], 0)
            )
            dq_acc[:, here] = dq
            own[0, :, here] = dk[:cells]
            own[1, :, here] = dv[:cells]
            tx[: text // 8, :, here] = (dk[cells:] * scale).reshape(text // 8, 8, HDIM)
            tx[text // 8:, :, here] = dv[cells:].reshape(text // 8, 8, HDIM)

    def forward(g):
        for d in range(2):
            col_copy[g, d].wait()
        for d in range(2):
            for v in range(2):
                c = remote(
                    hcol.at[g, :, d, v * (bands - 1)], hcor.at[g, :, 1 - v, d],
                    cor_s.at[g, d, v], cor_r.at[g, d, 1 - v], ha_of[v],
                )
                c.start()
                cor_copy[g, d, v] = c

    def halo(g):
        for v in range(2):
            for kv in range(2):
                row_copy[g, v, kv].wait()
            for d in range(2):
                cor_copy[g, d, v].wait()
        for h in range(per):
            here = slice(h * HDIM, (h + 1) * HDIM)
            absolute = slice((g * per + h) * HDIM, (g * per + h + 1) * HDIM)
            sides = []
            for kv in range(2):
                pieces = []
                for v in range(2):
                    pieces.append(to_rows(hrow[g, kv, v, :, :, :, here], frames * HALO * tile))
                    pieces.append(to_rows(hcor[g, kv, v, :, :, here], 2 * frames * HALO * HALO))
                pieces.append(to_rows(hcol[g, kv, :, :, :, here], border))
                sides.append(jnp.concatenate(pieces, 0).astype(BF16))
            dq, dk, dv = attend(sides[0], sides[1], g * per + h, lambda p: p * mask[...])
            dq_acc[:, absolute] += dq
            ret[g, 0, :, :, here] = dk.reshape(ret.shape[2], 8, HDIM)
            ret[g, 1, :, :, here] = dv.reshape(ret.shape[2], 8, HDIM)
        for v in range(2):
            c = remote(ret.at[g, :, 6 * v:6 * v + 6], rrow.at[g, 1 - v], rr_s.at[g, v], rr_r.at[g, 1 - v], ha_of[v])
            c.start()
            rr_copy[g, v] = c
        dq_ref[:, :, :, cols(g)] = (dq_acc[:, cols(g)] * scale).reshape(frames, tile, tile, part).astype(BF16)

    def fold_rows(g):
        for v in range(2):
            rr_copy[g, v].wait()
        for v in range(2):
            for kv in range(2):
                for d in range(2):
                    ret[g, kv, 12 + 4 * d + 3 * v] += rrow[g, v, kv, 4 + d]
        for d in range(2):
            c = remote(
                ret.at[g, :, 12 + 4 * d:16 + 4 * d], rcol.at[g, :, 1 - d],
                rc_s.at[g, d], rc_r.at[g, 1 - d], wa_of[d],
            )
            c.start()
            rc_copy[g, d] = c
        for v in range(2):
            for kv in range(2):
                for f in range(frames):
                    lo = f * tile * tile + v * (tile - HALO) * tile
                    own[kv, lo:lo + HALO * tile, cols(g)] += rrow[g, v, kv, 2 * f:2 * f + 2].reshape(HALO * tile, part)

    def fold_cols(g):
        for d in range(2):
            rc_copy[g, d].wait()
        for kv, out in enumerate((dk_ref, dv_ref)):
            came = rcol[g, kv].reshape(border, part)
            first = came.astype(BF16)
            left = came - first.astype(F32)
            second = left.astype(BF16)
            third = (left - second.astype(F32)).astype(BF16)
            total = own[kv, :, cols(g)] + contract(
                put_back, jnp.concatenate([first, second, third], 0), ((1,), (0,))
            )
            if kv == 0:
                total = total * scale
            out[:, :, :, cols(g)] = total.reshape(frames, tile, tile, part).astype(BF16)

    region = {"row": 0, "rows": 2 * text // 8, "col": 0, "cols": width}
    sums, regions = [], []

    def text_send(i):
        _, _, rows, wide, how = plan[i]
        regions.append(dict(region))
        row, col, bit = region["row"], region["col"], bits[i]
        send_row, send_col = row, col
        if how == "rows":
            send_row = row + (1 - bit) * rows
            region.update(row=row + bit * rows, rows=rows)
        elif how == "cols":
            send_col = col + (1 - bit) * wide
            region.update(col=col + bit * wide, cols=wide)
        c = remote(area(tx, send_row, rows, send_col, wide), trecv[i], t_s.at[i], t_r.at[i], partners[i])
        c.start()
        sums.append(c)

    def area(ref, row, rows, col, wide):
        lanes = pl.ds(pl.multiple_of(col, 128), wide) if not isinstance(col, int) else pl.ds(col, wide)
        return ref.at[pl.ds(row, rows), :, lanes]

    def mine(ref):
        return area(ref, region["row"], region["rows"], region["col"], region["cols"])

    def text_add(i):
        sums[i].wait()
        kept = mine(tx)
        kept[...] += trecv[i][...]

    gathers = []

    def text_spread(i):
        if i == len(plan) - 1:
            mine(tb)[...] = mine(tx)[...].astype(BF16)
        if plan[i][4] == "none":
            gathers.append(None)
            return
        c = remote(mine(tb), mine(tb), u_s.at[i], u_r.at[i], partners[i])
        c.start()
        gathers.append(c)

    def text_join(i):
        c = gathers.pop()
        if c is not None:
            c.wait()
        region.update(regions[i])

    steps = []
    for i in range(len(plan)):
        steps += [functools.partial(text_send, i), functools.partial(text_add, i)]
    for i in reversed(range(len(plan))):
        steps += [functools.partial(text_spread, i), functools.partial(text_join, i)]
    waiting = []
    for n in range(0, len(steps)):
        if n % 2 == 0:
            waiting.append([steps[n]])
            if n > 0:
                waiting[-1].insert(0, steps[n - 1])
    waiting.append([steps[-1]])

    def text_step():
        if waiting:
            for step in waiting.pop(0):
                step()

    local(0)
    local(1)
    forward(0)
    for g in range(2, GROUPS):
        local(g)
    text_step()
    forward(1)
    halo(0)
    text_step()
    for g in range(1, GROUPS):
        if g + 1 < GROUPS:
            forward(g + 1)
        halo(g)
        text_step()
        fold_rows(g - 1)
        text_step()
    fold_rows(GROUPS - 1)
    for g in range(GROUPS):
        text_step()
        fold_cols(g)
    while waiting:
        text_step()
    dtk_ref[...] = to_rows(tb[: text // 8], text).astype(BF16)
    dtv_ref[...] = to_rows(tb[text // 8:], text).astype(BF16)


def solution(mesh):
    n_ha, n_wa = mesh.shape["ha"], mesh.shape["wa"]

    def local(queries, keys, values, out_grad, log_norm, delta_rows, text_keys, text_values, window_table):
        frames, tile, _, width = queries.shape
        heads = width // HDIM
        text = text_keys.shape[0]
        cells = frames * tile * tile
        part = width // GROUPS
        bands = tile // HALO
        block = frames * HALO * HALO
        halo_blocks = (4 * HALO * tile * frames + 4 * block) // 8
        plan = text_plan(n_ha, n_wa, 2 * text // 8, width)
        received = []
        for _, _, rows, wide, _ in plan:
            received.append(pltpu.VMEM((rows, 8, wide), F32))
        sem = pltpu.SemaphoreType.DMA
        vmem = pl.BlockSpec(memory_space=pltpu.VMEM)
        outs = (
            jax.ShapeDtypeStruct(queries.shape, BF16),
            jax.ShapeDtypeStruct(queries.shape, BF16),
            jax.ShapeDtypeStruct(queries.shape, BF16),
            jax.ShapeDtypeStruct(text_keys.shape, BF16),
            jax.ShapeDtypeStruct(text_keys.shape, BF16),
        )
        return pl.pallas_call(
            functools.partial(kernel, n_ha, n_wa, plan),
            out_shape=outs,
            in_specs=[pl.BlockSpec(memory_space=pltpu.SMEM)] + [vmem] * 8,
            out_specs=[vmem] * 5,
            scratch_shapes=[
                pltpu.VMEM((GROUPS, 2, 2, bands, block, part), BF16),
                pltpu.VMEM((GROUPS, 2, 2, bands, block, part), BF16),
                pltpu.VMEM((GROUPS, 2, 2, frames, HALO, tile, part), BF16),
                pltpu.VMEM((GROUPS, 2, 2, 2, block, part), BF16),
                pltpu.VMEM((GROUPS, 2, halo_blocks, 8, part), F32),
                pltpu.VMEM((GROUPS, 2, 2, 6, 8, part), F32),
                pltpu.VMEM((GROUPS, 2, 2, bands, block, part), F32),
                pltpu.VMEM((2, cells, width), F32),
                pltpu.VMEM((cells, width), F32),
                pltpu.VMEM((8 * halo_blocks, cells), F32),
                pltpu.VMEM((heads, cells), F32),
                pltpu.VMEM((heads, cells), F32),
                pltpu.VMEM((2 * text // 8, 8, width), F32),
                pltpu.VMEM((2 * text // 8, 8, width), BF16),
                *received,
                sem((GROUPS, 2)), sem((GROUPS, 2)),
                sem((GROUPS, 2, 2)), sem((GROUPS, 2, 2)),
                sem((GROUPS, 2, 2)), sem((GROUPS, 2, 2)),
                sem((GROUPS, 2)), sem((GROUPS, 2)),
                sem((GROUPS, 2)), sem((GROUPS, 2)),
                sem((len(plan),)), sem((len(plan),)),
                sem((len(plan),)), sem((len(plan),)),
            ],
            compiler_params=pltpu.CompilerParams(
                collective_id=0, has_side_effects=True, vmem_limit_bytes=56 * 1024 * 1024
            ),
        )(
            window_table, queries, keys, values, out_grad,
            log_norm.reshape(-1, tile), delta_rows.reshape(-1, tile), text_keys, text_values,
        )

    tile_spec = P("group", "ha", "wa", None)
    stat_spec = P(None, "group", "ha", "wa")
    text_spec = P("group", None)
    return jax.shard_map(
        local,
        mesh=mesh,
        in_specs=(tile_spec,) * 4 + (stat_spec,) * 2 + (text_spec,) * 2 + (P(),),
        out_specs=(tile_spec,) * 3 + (text_spec,) * 2,
        check_vma=False,
    )
```

```python
import functools
import math

import jax
import jax.numpy as jnp
from jax import lax
from jax.experimental import pallas as pl
from jax.experimental.pallas import tpu as pltpu
from jax.sharding import PartitionSpec as P

HDIM = 128
HALO = 2
GROUPS = 4
MESH = pl.DeviceIdType.MESH
F32 = jnp.float32
BF16 = jnp.bfloat16


def text_plan(n_ha, n_wa, blocks, width):
    plan = []
    for axis, count in (("ha", n_ha), ("wa", n_wa)):
        far = 1
        while far < count:
            if blocks > 1:
                blocks //= 2
                plan.append((axis, far, blocks, width, "rows"))
            elif width % 256 == 0:
                width //= 2
                plan.append((axis, far, blocks, width, "cols"))
            else:
                plan.append((axis, far, blocks, width, "none"))
            far *= 2
    return plan


def to_rows(block, rows):
    return block.astype(F32).reshape(rows, block.shape[-1])


def contract(a, b, dims):
    return lax.dot_general(a, b, (dims, ((), ())), preferred_element_type=F32)


def kernel(
    n_ha, n_wa, plan,
    table, q_ref, k_ref, v_ref, g_ref, norm_ref, delta_ref, tk_ref, tv_ref,
    dq_ref, dk_ref, dv_ref, dtk_ref, dtv_ref,
    stage, hcol, hrow, hcor, ret, rrow, rcor, rcol, own, dq_acc, mask, norm, delta, tx, tb, *rest,
):
    trecv = rest[: len(plan)]
    (col_s, col_r, row_s, row_r, cor_s, cor_r, rr_s, rr_r, rc_s, rc_r, mid_s, mid_r, rq_s, rq_r, t_s, t_r, u_s, u_r) = rest[len(plan):]
    frames, tile, _, width = q_ref.shape
    cells = frames * tile * tile
    text = tk_ref.shape[0]
    heads = width // HDIM
    part = width // GROUPS
    per = heads // GROUPS
    bands = tile // HALO
    rim = ret.shape[2] - 2 * bands
    scale = 1.0 / math.sqrt(HDIM)
    ha, wa = lax.axis_index("ha"), lax.axis_index("wa")
    ha_of = [{"ha": lax.rem(ha + n_ha - 1, n_ha)}, {"ha": lax.rem(ha + 1, n_ha)}]
    wa_of = [{"wa": lax.rem(wa + n_wa - 1, n_wa)}, {"wa": lax.rem(wa + 1, n_wa)}]
    partners, bits = [], []
    for axis, far, _, _, _ in plan:
        at = ha if axis == "ha" else wa
        bit = lax.rem(lax.div(at, far), 2)
        bits.append(bit)
        partners.append({axis: at + far * (1 - 2 * bit)})

    barrier = pltpu.get_barrier_semaphore()
    greeted = ha_of + wa_of + partners
    for other in greeted:
        pl.semaphore_signal(barrier, inc=1, device_id=other, device_id_type=MESH)

    def cols(g):
        return slice(g * part, (g + 1) * part)

    def remote(src, dst, s, r, device):
        return pltpu.make_async_remote_copy(
            src_ref=src, dst_ref=dst, send_sem=s, recv_sem=r, device_id=device, device_id_type=MESH
        )

    border = 2 * bands * frames * HALO * HALO

    def cell_of(j):
        side = lax.div(j, border // 2)
        band = lax.rem(lax.div(j, frames * HALO * HALO), bands)
        frame = lax.rem(lax.div(j, HALO * HALO), frames)
        row = band * HALO + lax.rem(lax.div(j, HALO), HALO)
        col = lax.rem(j, HALO) + side * (tile - HALO)
        return frame * tile * tile + row * tile + col

    lane = lax.broadcasted_iota(jnp.int32, (border, cells), 1)
    pick = (lane == cell_of(lax.broadcasted_iota(jnp.int32, (border, cells), 0))).astype(F32).astype(BF16)
    back_row = lax.broadcasted_iota(jnp.int32, (cells, 3 * border), 0)
    back_lane = lax.broadcasted_iota(jnp.int32, (cells, 3 * border), 1)
    put_back = (back_row == cell_of(lax.rem(back_lane, border))).astype(F32).astype(BF16)

    col_copy, row_copy, cor_copy, rr_copy, rc_copy, mid_copy, rq_copy = {}, {}, {}, {}, {}, {}, {}
    for g in range(GROUPS):
        for kv, ref in enumerate((k_ref, v_ref)):
            full = to_rows(ref[:, :, :, cols(g)], cells).astype(BF16)
            strip = contract(pick, full, ((1,), (0,)))
            stage[g, kv] = strip.reshape(2, bands, frames * HALO * HALO, part).astype(BF16)
        if g == 0:
            pl.semaphore_wait(barrier, len(greeted))
        for d in range(2):
            c = remote(stage.at[g, :, d], hcol.at[g, :, 1 - d], col_s.at[g, d], col_r.at[g, 1 - d], wa_of[d])
            c.start()
            col_copy[g, d] = c
        for v in range(2):
            for kv, ref in enumerate((k_ref, v_ref)):
                lo = v * (tile - HALO)
                c = remote(
                    ref.at[:, lo:lo + HALO, :, cols(g)], hrow.at[g, kv, 1 - v],
                    row_s.at[g, v, kv], row_r.at[g, 1 - v, kv], ha_of[v],
                )
                c.start()
                row_copy[g, v, kv] = c

    square = (cells, cells)
    same = (lax.broadcasted_iota(jnp.int32, square, 0) == lax.broadcasted_iota(jnp.int32, square, 1)).astype(F32)
    for src, dst in ((norm_ref, norm), (delta_ref, delta)):
        dst[...] = lax.dot_general(
            src[...], same, (((0,), (0,)), ((), ())), precision=lax.Precision.HIGHEST, preferred_element_type=F32
        )

    def live(block):
        return table[ha, wa, block].astype(F32)

    at = 0
    for block, rows in ((1, 32), (7, 32), (0, 8), (2, 8), (6, 8), (8, 8), (3, 32), (5, 32)):
        mask[at:at + rows, :] = jnp.full((rows, cells), live(block), F32)
        at += rows
    own_live = live(4)

    def attend(keys, values, h, masking):
        here = slice(h * HDIM, (h + 1) * HDIM)
        qh = to_rows(q_ref[:, :, :, here], cells).astype(BF16)
        gh = to_rows(g_ref[:, :, :, here], cells).astype(BF16)
        s = contract(keys, qh, ((1,), (1,))) * scale
        p = masking(jnp.exp(s - norm[h:h + 1, :]))
        dp = contract(values, gh, ((1,), (1,)))
        ds = (p * (dp - delta[h:h + 1, :])).astype(BF16)
        dv = contract(p.astype(BF16), gh, ((1,), (0,)))
        dk = contract(ds, qh, ((1,), (0,)))
        dq = contract(ds, keys, ((0,), (0,)))
        return dq, dk, dv

    def texts():
        for h in range(heads):
            here = slice(h * HDIM, (h + 1) * HDIM)
            dq, dk, dv = attend(tk_ref[:, here], tv_ref[:, here], h, lambda p: p)
            dq_acc[:, here] = dq
            tx[: text // 8, :, here] = (dk * scale).reshape(text // 8, 8, HDIM)
            tx[text // 8:, :, here] = dv.reshape(text // 8, 8, HDIM)

    def local(g):
        for h in range(g * per, (g + 1) * per):
            here = slice(h * HDIM, (h + 1) * HDIM)
            keys, values = (to_rows(ref[:, :, :, here], cells).astype(BF16) for ref in (k_ref, v_ref))
            dq, dk, dv = attend(keys, values, h, lambda p: p * own_live)
            dq_acc[:, here] += dq
            own[0, :, here] = dk
            own[1, :, here] = dv

    def forward(g):
        for d in range(2):
            col_copy[g, d].wait()
        for d in range(2):
            for v in range(2):
                c = remote(
                    hcol.at[g, :, d, v * (bands - 1)], hcor.at[g, :, 1 - v, d],
                    cor_s.at[g, d, v], cor_r.at[g, d, 1 - v], ha_of[v],
                )
                c.start()
                cor_copy[g, d, v] = c

    def columns(g):
        for h in range(per):
            here = slice(h * HDIM, (h + 1) * HDIM)
            absolute = slice((g * per + h) * HDIM, (g * per + h + 1) * HDIM)
            keys, values = (to_rows(hcol[g, kv, :, :, :, here], border).astype(BF16) for kv in range(2))
            dq, dk, dv = attend(keys, values, g * per + h, lambda p: p * mask[8 * rim:])
            dq_acc[:, absolute] += dq
            ret[g, 0, rim:, :, here] = dk.reshape(2 * bands, 8, HDIM)
            ret[g, 1, rim:, :, here] = dv.reshape(2 * bands, 8, HDIM)
        for d in range(2):
            lo = rim + d * bands
            c = remote(
                ret.at[g, :, lo + 1:lo + bands - 1], rcol.at[g, :, 1 - d, 1:bands - 1],
                mid_s.at[g, d], mid_r.at[g, 1 - d], wa_of[d],
            )
            c.start()
            mid_copy[g, d] = c

    def pieces_pass(g, refs_of, lo, size, weights):
        for h in range(per):
            here = slice(h * HDIM, (h + 1) * HDIM)
            absolute = slice((g * per + h) * HDIM, (g * per + h + 1) * HDIM)
            keys, values = (refs_of(kv, here).astype(BF16) for kv in range(2))
            dq, dk, dv = attend(keys, values, g * per + h, lambda p: p * weights)
            dq_acc[:, absolute] += dq
            ret[g, 0, lo:lo + size, :, here] = dk.reshape(size, 8, HDIM)
            ret[g, 1, lo:lo + size, :, here] = dv.reshape(size, 8, HDIM)

    def strips(g):
        for v in range(2):
            for kv in range(2):
                row_copy[g, v, kv].wait()
        wide = 2 * frames * HALO * tile
        pieces_pass(g, lambda kv, here: to_rows(hrow[g, kv, :, :, :, :, here], wide), 0, wide // 8, mask[:wide])
        half = wide // 16
        for v in range(2):
            c = remote(
                ret.at[g, :, half * v:half * (v + 1)], rrow.at[g, 1 - v], rr_s.at[g, v], rr_r.at[g, 1 - v], ha_of[v]
            )
            c.start()
            rr_copy[g, v] = c

    def corners(g):
        for v in range(2):
            for d in range(2):
                cor_copy[g, d, v].wait()
        pieces_pass(
            g, lambda kv, here: to_rows(hcor[g, kv, :, :, :, here], 32), rim - 4, 4, mask[8 * (rim - 4):8 * rim]
        )
        for v in range(2):
            c = remote(
                ret.at[g, :, rim - 4 + 2 * v:rim - 2 + 2 * v], rcor.at[g, 1 - v],
                rq_s.at[g, v], rq_r.at[g, 1 - v], ha_of[v],
            )
            c.start()
            rq_copy[g, v] = c

    def fold_corners(g):
        for v in range(2):
            rq_copy[g, v].wait()
        for v in range(2):
            for d in range(2):
                at = rim + bands * d + (bands - 1) * v
                for kv in range(2):
                    ret[g, kv, at] += rcor[g, v, kv, d]
                c = remote(
                    ret.at[g, :, at], rcol.at[g, :, 1 - d, v * (bands - 1)],
                    rc_s.at[g, d, v], rc_r.at[g, 1 - d, v], wa_of[d],
                )
                c.start()
                rc_copy[g, d, v] = c

    def fold_rows(g):
        for v in range(2):
            rr_copy[g, v].wait()
        for v in range(2):
            for kv in range(2):
                for f in range(frames):
                    lo = f * tile * tile + v * (tile - HALO) * tile
                    own[kv, lo:lo + HALO * tile, cols(g)] += rrow[g, v, kv, 2 * f:2 * f + 2].reshape(HALO * tile, part)
        dq_ref[:, :, :, cols(g)] = (dq_acc[:, cols(g)] * scale).reshape(frames, tile, tile, part).astype(BF16)

    def fold_cols(g):
        for d in range(2):
            mid_copy[g, d].wait()
            for v in range(2):
                rc_copy[g, d, v].wait()
        for kv, out in enumerate((dk_ref, dv_ref)):
            came = rcol[g, kv].reshape(border, part)
            first = came.astype(BF16)
            left = came - first.astype(F32)
            second = left.astype(BF16)
            third = (left - second.astype(F32)).astype(BF16)
            total = own[kv, :, cols(g)] + contract(
                put_back, jnp.concatenate([first, second, third], 0), ((1,), (0,))
            )
            if kv == 0:
                total = total * scale
            out[:, :, :, cols(g)] = total.reshape(frames, tile, tile, part).astype(BF16)

    region = {"row": 0, "rows": 2 * text // 8, "col": 0, "cols": width}
    sums, regions = [], []

    def text_send(i):
        _, _, rows, wide, how = plan[i]
        regions.append(dict(region))
        row, col, bit = region["row"], region["col"], bits[i]
        send_row, send_col = row, col
        if how == "rows":
            send_row = row + (1 - bit) * rows
            region.update(row=row + bit * rows, rows=rows)
        elif how == "cols":
            send_col = col + (1 - bit) * wide
            region.update(col=col + bit * wide, cols=wide)
        c = remote(area(tx, send_row, rows, send_col, wide), trecv[i], t_s.at[i], t_r.at[i], partners[i])
        c.start()
        sums.append(c)

    def area(ref, row, rows, col, wide):
        lanes = pl.ds(pl.multiple_of(col, 128), wide) if not isinstance(col, int) else pl.ds(col, wide)
        return ref.at[pl.ds(row, rows), :, lanes]

    def mine(ref):
        return area(ref, region["row"], region["rows"], region["col"], region["cols"])

    def text_add(i):
        sums[i].wait()
        kept = mine(tx)
        kept[...] += trecv[i][...]

    gathers = []

    def text_spread(i):
        if i == len(plan) - 1:
            mine(tb)[...] = mine(tx)[...].astype(BF16)
        if plan[i][4] == "none":
            gathers.append(None)
            return
        c = remote(mine(tb), mine(tb), u_s.at[i], u_r.at[i], partners[i])
        c.start()
        gathers.append(c)

    def text_join(i):
        c = gathers.pop()
        if c is not None:
            c.wait()
        region.update(regions[i])

    steps = []
    for i in range(len(plan)):
        steps += [functools.partial(text_send, i), functools.partial(text_add, i)]
    for i in reversed(range(len(plan))):
        steps += [functools.partial(text_spread, i), functools.partial(text_join, i)]
    waiting = []
    for n in range(0, len(steps)):
        if n % 2 == 0:
            waiting.append([steps[n]])
            if n > 0:
                waiting[-1].insert(0, steps[n - 1])
    waiting.append([steps[-1]])

    def text_step():
        if waiting:
            for step in waiting.pop(0):
                step()

    texts()
    text_step()
    local(0)
    local(1)
    text_step()
    local(2)
    local(3)
    strips(0)
    strips(1)
    text_step()
    forward(0)
    columns(0)
    forward(1)
    columns(1)
    corners(0)
    text_step()
    forward(2)
    columns(2)
    corners(1)
    forward(3)
    columns(3)
    corners(2)
    text_step()
    fold_corners(0)
    corners(3)
    strips(2)
    fold_corners(1)
    strips(3)
    fold_corners(2)
    text_step()
    fold_corners(3)
    text_step()
    fold_rows(0)
    fold_rows(1)
    fold_rows(2)
    fold_rows(3)
    fold_cols(0)
    text_step()
    fold_cols(1)
    fold_cols(2)
    fold_cols(3)
    while waiting:
        text_step()
    dtk_ref[...] = to_rows(tb[: text // 8], text).astype(BF16)
    dtv_ref[...] = to_rows(tb[text // 8:], text).astype(BF16)


def hand_on(*refs):
    count = len(refs) // 2
    for source, target in zip(refs[:count], refs[count:]):
        target[...] = source[...]


def solution(mesh):
    n_ha, n_wa = mesh.shape["ha"], mesh.shape["wa"]

    def local(queries, keys, values, out_grad, log_norm, delta_rows, text_keys, text_values, window_table):
        frames, tile, _, width = queries.shape
        heads = width // HDIM
        text = text_keys.shape[0]
        cells = frames * tile * tile
        part = width // GROUPS
        bands = tile // HALO
        block = frames * HALO * HALO
        halo_blocks = (4 * HALO * tile * frames + 4 * block) // 8
        plan = text_plan(n_ha, n_wa, 2 * text // 8, width)
        received = []
        for _, _, rows, wide, _ in plan:
            received.append(pltpu.VMEM((rows, 8, wide), F32))
        sem = pltpu.SemaphoreType.DMA
        vmem = pl.BlockSpec(memory_space=pltpu.VMEM)
        outs = (
            jax.ShapeDtypeStruct(queries.shape, BF16),
            jax.ShapeDtypeStruct(queries.shape, BF16),
            jax.ShapeDtypeStruct(queries.shape, BF16),
            jax.ShapeDtypeStruct(text_keys.shape, BF16),
            jax.ShapeDtypeStruct(text_keys.shape, BF16),
        )
        results = pl.pallas_call(
            functools.partial(kernel, n_ha, n_wa, plan),
            out_shape=outs,
            in_specs=[pl.BlockSpec(memory_space=pltpu.SMEM)] + [vmem] * 8,
            out_specs=[vmem] * 5,
            scratch_shapes=[
                pltpu.VMEM((GROUPS, 2, 2, bands, block, part), BF16),
                pltpu.VMEM((GROUPS, 2, 2, bands, block, part), BF16),
                pltpu.VMEM((GROUPS, 2, 2, frames, HALO, tile, part), BF16),
                pltpu.VMEM((GROUPS, 2, 2, 2, block, part), BF16),
                pltpu.VMEM((GROUPS, 2, halo_blocks, 8, part), F32),
                pltpu.VMEM((GROUPS, 2, 2, 4, 8, part), F32),
                pltpu.VMEM((GROUPS, 2, 2, 2, 8, part), F32),
                pltpu.VMEM((GROUPS, 2, 2, bands, block, part), F32),
                pltpu.VMEM((2, cells, width), F32),
                pltpu.VMEM((cells, width), F32),
                pltpu.VMEM((8 * halo_blocks, cells), F32),
                pltpu.VMEM((heads, cells), F32),
                pltpu.VMEM((heads, cells), F32),
                pltpu.VMEM((2 * text // 8, 8, width), F32),
                pltpu.VMEM((2 * text // 8, 8, width), BF16),
                *received,
                sem((GROUPS, 2)), sem((GROUPS, 2)),
                sem((GROUPS, 2, 2)), sem((GROUPS, 2, 2)),
                sem((GROUPS, 2, 2)), sem((GROUPS, 2, 2)),
                sem((GROUPS, 2)), sem((GROUPS, 2)),
                sem((GROUPS, 2, 2)), sem((GROUPS, 2, 2)),
                sem((GROUPS, 2)), sem((GROUPS, 2)),
                sem((GROUPS, 2)), sem((GROUPS, 2)),
                sem((len(plan),)), sem((len(plan),)),
                sem((len(plan),)), sem((len(plan),)),
            ],
            compiler_params=pltpu.CompilerParams(
                collective_id=0, has_side_effects=True, vmem_limit_bytes=56 * 1024 * 1024
            ),
        )(
            window_table, queries, keys, values, out_grad,
            log_norm.transpose(1, 2, 3, 0).reshape(cells, heads), delta_rows.transpose(1, 2, 3, 0).reshape(cells, heads),
            text_keys, text_values,
        )

        return pl.pallas_call(
            hand_on,
            out_shape=outs,
            in_specs=[vmem] * 5,
            out_specs=[vmem] * 5,
        )(*results)

    tile_spec = P("group", "ha", "wa", None)
    stat_spec = P(None, "group", "ha", "wa")
    text_spec = P("group", None)
    return jax.shard_map(
        local,
        mesh=mesh,
        in_specs=(tile_spec,) * 4 + (stat_spec,) * 2 + (text_spec,) * 2 + (P(),),
        out_specs=(tile_spec,) * 3 + (text_spec,) * 2,
        check_vma=False,
    )
```
